1024 devices in a mesh: expert: 8 (over x, core), tensor: 128 (over z, y).
Axes of the slice: x: 4, y: 4, z: 32, core: 2. Of those that a mesh axis runs over, the one named last changes fastest.
Arguments:
- tokens: bfloat16 [256, 7168], P('expert', 'tensor'), may hold values from -6 to 6
- routes: int32 [256, 8], P('expert'), may hold values from 0 to 31, all different within a row; in each aligned block of 256 rows (0 to 255, 256 to 511, ...) at most 128 rows name the same one
- gates: bfloat16 [256, 8], P('expert'), may hold values from 0.099609375 to 0.59765625
- w_gate: bfloat16 [32, 2048, 7168], P('expert', 'tensor'), may hold values from -0.0625 to 0.0625
- w_up: bfloat16 [32, 2048, 7168], P('expert', 'tensor'), may hold values from -0.0625 to 0.0625
- w_down: bfloat16 [32, 2048, 7168], P('expert', None, 'tensor'), may hold values from -0.125 to 0.125
Outputs:
- moe_out: bfloat16 [256, 7168], P('expert', 'tensor')
The draws below stay inside these ranges and needn't reach their ends.
Inputs may be any that keep to these rules, and one draw needn't show every extreme that they name: `routes`: each row names 8 different experts. No expert is named by more than 128 of the 256 rows, and one expert is named by exactly 128 rows.
All inputs are finite; a program needn't handle non-finite values.
Results may differ from the reference program's by a relative error of at most 0.0049.
Values may be sent and summed in bfloat16 or wider, within the bound.
A program may use at most 32 MiB of HBM per device.

```python
import math
import jax
import jax.numpy as jnp
import numpy as np
from jax import lax

D = 7168
FF = 2048
TOPK = 8
EXPERTS = 32
TOKENS = 256
CAP = 128


def steps_of(own_key, extent, split, smallest, largest):
    def one(dim, blocks):
        steps = jax.random.uniform(jax.random.fold_in(jax.random.fold_in(own_key, 6), dim), (blocks,), jnp.float32, smallest / len(split), largest / len(split))
        return jnp.repeat(jnp.exp(steps), extent[dim] // blocks).reshape((-1,) + (1,) * (len(extent) - dim - 1))

    factor_of = one(*split[0])
    for cut in split[1:]:
        factor_of = factor_of * one(*cut)
    return factor_of


def shared_out(key, own, number, rows, count, top, limit, lean):
    ranking = jax.random.permutation(key, count)
    crowded, ordinary = load_shares(count, rows * top, limit, lean, True), load_shares(count, rows * top, limit, lean, False)
    places = jnp.arange(count)

    def named(sizes, offset_by):
        used = int((sizes > 0).sum())
        fixed = max(1, used // 4)
        passed = fixed + (places - fixed + offset_by * (used - fixed)) % max(1, count - fixed)
        return jnp.zeros((count,), jnp.int32).at[ranking[jnp.where(places < fixed, places, passed)]].set(jnp.asarray(sizes, jnp.int32))

    sizes = jnp.where(number % 4 == 0, named(crowded, number // 4), named(ordinary, number - number // 4 - 1))
    mixed = jax.random.permutation(jax.random.fold_in(own, 3), count)
    source_of, receiver = mixed[0:count // 2 * 2:2], mixed[1:count // 2 * 2:2]
    room = jnp.minimum(sizes[source_of] - 1, limit - sizes[receiver]) // 2
    room = jnp.where((source_of == ranking[0]) | (receiver == ranking[0]) | (sizes[receiver] == 0), 0, jnp.maximum(room, 0))
    passed = jax.random.randint(jax.random.fold_in(own, 4), (count // 2,), 0, 1 << 20) % (room + 1)
    sizes = sizes.at[source_of].add(-passed).at[receiver].add(passed)
    labels = jnp.searchsorted(jnp.cumsum(sizes), jnp.arange(rows * top), side="right").astype(jnp.int32)
    table = labels.reshape(top, rows).T
    table = table[jax.random.permutation(jax.random.fold_in(own, 1), rows)]
    offset_by = jax.random.randint(jax.random.fold_in(own, 2), (rows, 1), 0, top)
    return jnp.take_along_axis(table, (jnp.arange(top)[None, :] + offset_by) % top, axis=1)


def load_shares(count, total, limit, lean, full):
    weights = [(1 << 20) // math.isqrt(standing ** lean) + 1 for standing in range(1, count + 1)]
    largest = limit if full else min(limit, max(-(-total // count), total * weights[0] // sum(weights)))
    least = 1 if total - largest >= count - 1 else 0
    given, surplus = [largest] + [least] * (count - 1), total - largest - least * (count - 1)
    while surplus > 0:
        movable = [i for i in range(1, count) if given[i] < largest] or [i for i in range(1, count) if given[i] < limit]
        whole, remaining = sum([weights[i] for i in movable]), surplus
        for i in movable:
            more = min(limit - given[i], max(1, remaining * weights[i] // whole), surplus)
            given[i] = given[i] + more
            surplus = surplus - more
    return np.array(given)


def scatter_about(key, shape, width, bound, split=(), kind=jnp.bfloat16):
    values = width * jax.random.normal(key, shape, jnp.float32)
    if split:
        values = values * steps_of(key, shape, split, -0.22, 0.18)
    return jnp.clip(values, -bound, bound).astype(kind)


def setup_inputs(seed: int = 0) -> dict:
    arg_keys = jax.random.split(jax.random.key(seed), 7)
    tokens = scatter_about(arg_keys[0], (TOKENS, D), 1.0, 6.0, ((0, 8), (1, 128)))
    routes_keys = jax.random.split(jax.random.fold_in(arg_keys[1], 1), TOKENS // TOKENS)
    routes_turns = jax.random.permutation(jax.random.fold_in(arg_keys[1], 3), TOKENS // TOKENS)
    routes = jax.vmap(lambda own, number: shared_out(jax.random.fold_in(arg_keys[1], 2), own, number, TOKENS, EXPERTS, TOPK, CAP, 2))(routes_keys, routes_turns).reshape((TOKENS, TOPK))
    gates = jnp.clip(0.099609375 + 0.49804688 * jax.random.uniform(arg_keys[2], (TOKENS, TOPK), jnp.float32) ** steps_of(arg_keys[2], (TOKENS, TOPK), ((0, 8),), -0.2, 0.2), 0.099609375, 0.59765625).astype(jnp.bfloat16)
    w_gate = scatter_about(arg_keys[3], (EXPERTS, FF, D), D ** -0.5, 0.0625, ((0, 8), (1, 128)))
    w_up = scatter_about(arg_keys[4], (EXPERTS, FF, D), D ** -0.5, 0.0625, ((0, 8), (1, 128)))
    w_down = scatter_about(arg_keys[5], (EXPERTS, FF, D), FF ** -0.5, 0.125, ((0, 8), (2, 128)))
    return {"tokens": tokens, "routes": routes, "gates": gates, "w_gate": w_gate, "w_up": w_up, "w_down": w_down}


def reference(tokens, routes, gates, w_gate, w_up, w_down):
    expert_ids = jnp.arange(EXPERTS, dtype=jnp.int32)
    route_hits = routes[:, :, None] == expert_ids[None, None, :]
    member = jnp.sum(route_hits.astype(jnp.int32), axis=1)
    position = jnp.cumsum(member, axis=0) - member
    weights = jnp.sum(gates.astype(jnp.float32)[:, :, None] * route_hits.astype(jnp.float32), axis=1)
    slot_ids = jnp.arange(CAP, dtype=jnp.int32)

    def one_expert(running, packed):
        member_col, place_col, weight_col, gate_w, up_w, down_w = packed
        picked = (place_col[None, :] == slot_ids[:, None]) & (member_col[None, :] > 0)
        slot_rows = jnp.dot(picked.astype(jnp.bfloat16), tokens, preferred_element_type=jnp.float32).astype(jnp.bfloat16)
        gate_proj = lax.dot_general(slot_rows, gate_w, (((1,), (1,)), ((), ())), preferred_element_type=jnp.float32)
        up_proj = lax.dot_general(slot_rows, up_w, (((1,), (1,)), ((), ())), preferred_element_type=jnp.float32)
        hidden = (jax.nn.silu(gate_proj) * up_proj).astype(jnp.bfloat16)
        expert_out = jnp.dot(hidden, down_w, preferred_element_type=jnp.float32)
        mixing = picked.astype(jnp.float32).T * weight_col[:, None]
        return running + jnp.dot(mixing, expert_out, precision=lax.Precision.HIGHEST), None

    start = jnp.zeros((tokens.shape[0], tokens.shape[1]), jnp.float32)
    running, _ = lax.scan(one_expert, start, (member.T, position.T, weights.T, w_gate, w_up, w_down))
    return running.astype(jnp.bfloat16)
```

```python
import functools

import jax
import jax.numpy as jnp
from jax import lax
from jax.experimental import pallas as pl
from jax.experimental.pallas import tpu as pltpu
from jax.sharding import Mesh
from jax.sharding import PartitionSpec as P

CAP = 128
FEAT = 56
ROWS = 16
HID = 16
LOCAL = 4
NEAR = (0, -2, -1, 1)
F32 = jnp.float32
BF16 = jnp.bfloat16
MESH = pl.DeviceIdType.MESH


def iota(shape, dim):
    return lax.broadcasted_iota(jnp.int32, shape, dim)


def ones_where(cond):
    return jnp.where(cond, 1.0, 0.0).astype(BF16)


def dot(a, b):
    return jnp.dot(a, b, preferred_element_type=F32)


def dot_nt(a, b):
    return lax.dot_general(a, b, (((1,), (1,)), ((), ())), preferred_element_type=F32)


def body(sizes, *refs):
    (tok_ref, routes_ref, gates_ref, wg_hbm, wu_hbm, wd_hbm, out_ref,
     xbuf, hbuf, wv, wp, wdv, wdt, pick, acc, yt, pt, mix, comb, rbuf,
     load_sem, xs, xr_, hs, hr, es, er) = refs
    nx, nz, ny = sizes
    top = nz // 8
    x, c = lax.axis_index("x"), lax.axis_index("c")
    z, y = lax.axis_index("z"), lax.axis_index("y")

    def at_x(d):
        return {"x": lax.rem(x + d, nx)}

    def at_y(d):
        return {"y": lax.rem(y + d, ny)}

    def at_z(d):
        return {"z": lax.rem(z + d + nz, nz)}

    def dirs(k):
        return 1 if k in (0, top) else 2

    def start_of(k):
        return 0 if k == 0 else 4 + 8 * (k - 1)

    def part(k, first, count):
        n = dirs(k)
        return pl.ds(start_of(k) + first * n, count * n)

    def one(k, near, way):
        return start_of(k) + near * dirs(k) + way

    def shift_of(k, near, way):
        return NEAR[near] + (4 * k if way or k == top else -4 * k)

    def send(src, dst, send_sem, recv_sem, where):
        pltpu.make_async_remote_copy(
            src_ref=src, dst_ref=dst, send_sem=send_sem, recv_sem=recv_sem,
            device_id=where, device_id_type=MESH,
        ).start()

    def wait(region, sem):
        pltpu.make_async_copy(region, region, sem).wait()

    loads = [
        pltpu.make_async_copy(wg_hbm, wv.at[pl.ds(0, LOCAL)], load_sem.at[0]),
        pltpu.make_async_copy(wu_hbm, wv.at[pl.ds(LOCAL, LOCAL)], load_sem.at[1]),
        pltpu.make_async_copy(wd_hbm, wdv, load_sem.at[2]),
    ]
    for load in loads:
        load.start()

    barrier = pltpu.get_barrier_semaphore()
    peers = [at_z(d) for d in (4, -4, 1, -1, 2, -2)]
    peers += [at_y(d) for d in range(1, ny)]
    peers += [at_x(d) for d in range(1, nx)]
    peers += [{"c": 1 - c}] + [{**at_x(d), "c": 1 - c} for d in range(1, nx)]
    for peer in peers:
        pl.semaphore_signal(barrier, inc=1, device_id=peer, device_id_type=MESH)

    even = (y % 2) == 0
    meta = jnp.where(
        even, routes_ref[...].astype(F32), gates_ref[...].astype(F32)
    ).astype(BF16)
    tile = jnp.zeros((ROWS, 128), F32)
    for half in range(2):
        rows = pl.ds(half * ROWS, ROWS)
        k, lane = iota((FEAT, 128), 0), iota((FEAT, 128), 1)
        tile += dot(tok_ref[rows, :], ones_where(k + 64 * half == lane))
        k, lane = iota((8, 128), 0), iota((8, 128), 1)
        tile += dot(
            meta[half * ROWS:(half + 1) * ROWS], ones_where(k + FEAT + 64 * half == lane)
        )
    xbuf[0, 0, 0, 0] = tile.astype(BF16)

    pl.semaphore_wait(barrier, len(peers))

    def x_far_send(k):
        if k < top:
            send(xbuf.at[0, 0, 0, one(k - 1, 0, 0)], xbuf.at[0, 0, 0, one(k, 0, 0)],
                 xs.at[k, 0], xr_.at[k, 0], at_z(4))
            send(xbuf.at[0, 0, 0, one(k - 1, 0, dirs(k - 1) - 1)],
                 xbuf.at[0, 0, 0, one(k, 0, 1)], xs.at[k, 0], xr_.at[k, 0], at_z(-4))
        else:
            send(xbuf.at[0, 0, 0, one(k - 1, 0, 0)], xbuf.at[0, 0, 0, one(k, 0, 0)],
                 xs.at[k, 0], xr_.at[k, 0], at_z(4))

    def x_far_region(k):
        return xbuf.at[0, 0, 0, part(k, 0, 1)]

    def x_near_send(k):
        for near, d in ((1, 2), (2, 1), (3, -1)):
            send(xbuf.at[0, 0, 0, part(k, 0, 1)], xbuf.at[0, 0, 0, part(k, near, 1)],
                 xs.at[k, 1], xr_.at[k, 1], at_z(d))

    def x_near_region(k):
        return xbuf.at[0, 0, 0, part(k, 1, 3)]

    def x_first_send(k):
        a, b = part(k, 0, 2), part(k, 2, 2)
        for d in range(1, ny):
            send(xbuf.at[0, 0, 0, a], xbuf.at[0, 0, ny - d, a],
                 xs.at[k, 2], xr_.at[k, 2], at_y(d))
        for d in range(1, nx):
            send(xbuf.at[0, 0, 0, b], xbuf.at[0, nx - d, 0, b],
                 xs.at[k, 3], xr_.at[k, 3], at_x(d))

    def x_first_regions(k):
        return (
            xbuf.at[0, 0, pl.ds(1, ny - 1), part(k, 0, 2)],
            xbuf.at[0, pl.ds(1, nx - 1), 0, part(k, 2, 2)],
        )

    def x_second_send(k):
        a, b = part(k, 0, 2), part(k, 2, 2)
        for d in range(1, nx):
            send(xbuf.at[0, 0, :, a], xbuf.at[0, nx - d, :, a],
                 xs.at[k, 4], xr_.at[k, 4], at_x(d))
        for d in range(1, ny):
            send(xbuf.at[0, :, 0, b], xbuf.at[0, :, ny - d, b],
                 xs.at[k, 5], xr_.at[k, 5], at_y(d))

    def x_second_regions(k):
        return (
            xbuf.at[0, pl.ds(1, nx - 1), :, part(k, 0, 2)],
            xbuf.at[0, :, pl.ds(1, ny - 1), part(k, 2, 2)],
        )

    def x_core_send(k):
        g = part(k, 0, 4)
        send(xbuf.at[0, :, :, g], xbuf.at[1, :, :, g],
             xs.at[k, 6], xr_.at[k, 6], {"c": 1 - c})

    def x_core_region(k):
        return xbuf.at[1, :, :, part(k, 0, 4)]

    lanes = 2 * nx * ROWS

    def tile_rows(yr, zi):
        return xbuf[:, :, yr, zi].reshape(lanes, 128)

    def gate_up(k):
        def step(yr, carry):
            total = None
            col = lax.rem(y + yr, ny)
            entries = [(near, way) for near in range(4) for way in range(dirs(k))]
            for p in range(0, len(entries), 2):
                left, right = [], []
                for near, way in entries[p:p + 2]:
                    t = lax.rem(z + shift_of(k, near, way) + nz, nz) * ny + col
                    left.append(wp[t].reshape(256, 128))
                    right.append(tile_rows(yr, one(k, near, way)))
                term = dot_nt(
                    jnp.concatenate(left, axis=1), jnp.concatenate(right, axis=1)
                )
                total = term if total is None else total + term
            acc[...] += total
            return carry

        lax.fori_loop(0, ny, step, 0)

    def prepare_gate_up(i):
        start = FEAT * i
        base, off = start // 128 * 128, start % 128
        width = 128 if off + FEAT <= 128 else 256
        k, lane = iota((width, 256), 0), iota((width, 256), 1)
        j = jnp.where(lane < 128, lane, lane - 192)
        pick[pl.ds(0, width), :] = ones_where((k == j + off) & (j >= 0) & (j < FEAT))

        def step(q, carry):
            cols = pl.ds(pl.multiple_of(q * (16 * FEAT) + base, 128), width)
            got = dot(
                wv[:, :, cols].reshape(2 * LOCAL * HID, width), pick[pl.ds(0, width), :]
            ).astype(BF16)
            wp[q * 16 + i, 0] = got[:, :128]
            wp[q * 16 + i, 1] = got[:, 128:]
            return carry

        lax.fori_loop(0, nz * ny // 16, step, 0)

    def prepare_down(k):
        eye = ones_where(iota((64, FEAT), 0) == iota((64, FEAT), 1))

        def step(e, carry):
            for way in range(dirs(k)):
                rows = []
                for yr in range(ny):
                    for near in range(4):
                        t = lax.rem(z + shift_of(k, near, way) + nz, nz) * ny
                        t = t + lax.rem(y + yr, ny)
                        f = pl.multiple_of(t * HID, HID)
                        rows.append(wdv[e, pl.ds(f, HID), :])
                turned = dot_nt(eye, jnp.concatenate(rows, axis=0))
                wdt[2 * k - (1 if k else 0) + way, e] = turned.astype(BF16)
            return carry

        lax.fori_loop(0, LOCAL, step, 0)

    def prepare_slots():
        r_at = lax.rem(y, 2)
        routes = tile_rows(r_at, 0).astype(F32)
        gates = tile_rows(1 - r_at, 0).astype(F32)
        n = 2 * lanes

        def token_of(i):
            half, i = i // lanes, lax.rem(i, lanes)
            cr, i = i // (nx * ROWS), lax.rem(i, nx * ROWS)
            xr, r = i // ROWS, lax.rem(i, ROWS)
            e = lax.rem(x + xr, nx) * 2 + (c + cr * (1 - 2 * c))
            return e * 32 + half * ROWS + r

        before = ones_where(token_of(iota((n, n), 1)) < token_of(iota((n, n), 0)))
        sel = []
        for half in range(2):
            k = iota((128, 128), 0)
            low = FEAT + 64 * half
            sel.append(ones_where((k >= low) & (k < low + 8)))
        slot_of = iota((n, CAP), 1).astype(F32)
        for e in range(LOCAL):
            name = ((x * 2 + c) * LOCAL + e).astype(F32)
            hit = routes == name
            hit_one = ones_where(hit)
            hit_gate = jnp.where(hit, gates, 0.0).astype(BF16)
            member = jnp.concatenate([dot(hit_one, s) for s in sel], axis=0)
            weight = jnp.concatenate([dot(hit_gate, s) for s in sel], axis=0)
            slot = dot(before, member.astype(BF16))
            picked = (member > 0.5) & (slot == slot_of)
            pt[e] = ones_where(picked)
            mix[:, pl.ds(e * CAP, CAP)] = jnp.where(picked, weight, 0.0).astype(BF16)

    acc[...] = jnp.zeros_like(acc)
    x_far_send(1)
    x_near_send(0)
    loads[0].wait()
    loads[1].wait()
    for tick in range(1, top + 6):
        if tick <= 4:
            for i in range(4 * (tick - 1), 4 * tick):
                prepare_gate_up(i)
        g = tick - 1
        if 0 <= g <= top:
            wait(x_near_region(g), xr_.at[g, 1])
            x_first_send(g)
        g = tick - 2
        if 0 <= g <= top:
            for j, region in enumerate(x_first_regions(g)):
                wait(region, xr_.at[g, 2 + j])
            x_second_send(g)
        g = tick - 3
        if 0 <= g <= top:
            for j, region in enumerate(x_second_regions(g)):
                wait(region, xr_.at[g, 4 + j])
            x_core_send(g)
        if tick <= top:
            wait(x_far_region(tick), xr_.at[tick, 0])
            if tick < top:
                x_far_send(tick + 1)
            x_near_send(tick)
        g = tick - 4
        if 0 <= g <= top:
            wait(x_core_region(g), xr_.at[g, 6])
            if g == 0:
                prepare_slots()
            gate_up(g)
        g = tick - 5
        if g == 0:
            loads[2].wait()

    parts = []
    for half in range(2):
        gate = acc[pl.ds(half * 128, 64), :]
        up = acc[pl.ds(half * 128 + 64, 64), :]
        parts.append((gate / (1.0 + jnp.exp(-gate)) * up).astype(BF16))
    hidden = jnp.concatenate(parts, axis=1)
    for e in range(LOCAL):
        hbuf[0, 0, e] = dot(hidden[e * HID:(e + 1) * HID], pt[e]).astype(BF16)

    ea, eb = pl.ds(0, 3), pl.ds(3, 1)

    def h_far_send(k):
        if k < top:
            send(hbuf.at[0, one(k - 1, 0, 0)], hbuf.at[0, one(k, 0, 0)],
                 hs.at[k, 0], hr.at[k, 0], at_z(4))
            send(hbuf.at[0, one(k - 1, 0, dirs(k - 1) - 1)], hbuf.at[0, one(k, 0, 1)],
                 hs.at[k, 0], hr.at[k, 0], at_z(-4))
        else:
            for way, e, d in ((0, 0, 4), (1, 2, -4)):
                way = min(way, dirs(k - 1) - 1)
                send(hbuf.at[0, one(k - 1, 0, way), pl.ds(e, 2)],
                     hbuf.at[0, one(k, 0, 0), pl.ds(e, 2)],
                     hs.at[k, 0], hr.at[k, 0], at_z(d))

    def h_far_region(k):
        return hbuf.at[0, part(k, 0, 1)]

    def h_first_send(k):
        own = part(k, 0, 1)
        for near, d in ((1, 2), (2, 1), (3, -1)):
            send(hbuf.at[0, own, ea], hbuf.at[0, part(k, near, 1), ea],
                 hs.at[k, 1], hr.at[k, 1], at_z(d))
        for d in range(1, ny):
            send(hbuf.at[0, own, eb], hbuf.at[ny - d, own, eb],
                 hs.at[k, 2], hr.at[k, 2], at_y(d))

    def h_first_regions(k):
        return (
            hbuf.at[0, part(k, 1, 3), ea],
            hbuf.at[pl.ds(1, ny - 1), part(k, 0, 1), eb],
        )

    def h_second_send(k):
        own, group = part(k, 0, 1), part(k, 0, 4)
        for d in range(1, ny):
            send(hbuf.at[0, group, ea], hbuf.at[ny - d, group, ea],
                 hs.at[k, 3], hr.at[k, 3], at_y(d))
        for near, d in ((1, 2), (2, 1), (3, -1)):
            send(hbuf.at[:, own, eb], hbuf.at[:, part(k, near, 1), eb],
                 hs.at[k, 4], hr.at[k, 4], at_z(d))

    def h_second_regions(k):
        return (
            hbuf.at[pl.ds(1, ny - 1), part(k, 0, 4), ea],
            hbuf.at[:, part(k, 1, 3), eb],
        )

    def down(k):
        def step(e, carry):
            total = yt[e]
            for way in range(dirs(k)):
                rows = [
                    hbuf[yr, one(k, near, way), e]
                    for yr in range(ny) for near in range(4)
                ]
                total += dot(
                    wdt[2 * k - (1 if k else 0) + way, e], jnp.concatenate(rows, axis=0)
                )
            yt[e] = total
            return carry

        lax.fori_loop(0, LOCAL, step, 0)

    yt[...] = jnp.zeros_like(yt)
    h_far_send(1)
    h_first_send(0)
    for tick in range(1, top + 3):
        if tick == 1:
            for k in range(top + 1):
                prepare_down(k)
        g = tick - 1
        if 0 <= g <= top:
            for j, region in enumerate(h_first_regions(g)):
                wait(region, hr.at[g, 1 + j])
            h_second_send(g)
        if tick <= top:
            wait(h_far_region(tick), hr.at[tick, 0])
            if tick < top:
                h_far_send(tick + 1)
            h_first_send(tick)
        g = tick - 2
        if 0 <= g <= top:
            for j, region in enumerate(h_second_regions(g)):
                wait(region, hr.at[g, 3 + j])
            down(g)

    y_all = jnp.concatenate([yt[e] for e in range(LOCAL)], axis=1)
    high = y_all.astype(BF16)
    low = (y_all - high.astype(F32)).astype(BF16)
    none = jnp.zeros_like(high)
    total = jnp.zeros((lanes, 128), F32)
    for half in range(2):
        weights = mix[pl.ds(half * lanes, lanes), :]
        for term in (high, low):
            pair = (term, none) if half == 0 else (none, term)
            total += dot_nt(weights, jnp.concatenate(pair, axis=0))
    comb[...] = total.reshape(2 * nx, ROWS, 128)
    for j in range(1, 2 * nx):
        cr, xr = j // nx, j % nx
        where = {"c": 1 - c} if cr else {}
        if xr:
            where = {**where, **at_x(xr)}
        send(comb.at[j], rbuf.at[cr * nx + (nx - xr) % nx], es.at[0], er.at[0], where)
    rest = pl.ds(1, 2 * nx - 1)
    wait(rbuf.at[rest], er.at[0])
    total = comb[0]
    for j in range(1, 2 * nx):
        total += rbuf[j]
    out_ref[pl.ds(0, ROWS), :] = total[:, :FEAT].astype(BF16)
    out_ref[pl.ds(ROWS, ROWS), :] = pltpu.roll(total, 64, 1)[:, :FEAT].astype(BF16)

    for k in range(top + 1):
        if k:
            wait(x_far_region(k), xs.at[k, 0])
            wait(h_far_region(k), hs.at[k, 0])
        wait(x_near_region(k), xs.at[k, 1])
        for j, region in enumerate(x_first_regions(k)):
            wait(region, xs.at[k, 2 + j])
        for j, region in enumerate(x_second_regions(k)):
            wait(region, xs.at[k, 4 + j])
        wait(x_core_region(k), xs.at[k, 6])
        for j, region in enumerate(h_first_regions(k)):
            wait(region, hs.at[k, 1 + j])
        for j, region in enumerate(h_second_regions(k)):
            wait(region, hs.at[k, 3 + j])
    wait(comb.at[rest], es.at[0])


def on_device(sizes, *args):
    nx, nz, ny = sizes
    top = nz // 8
    features = nz * ny * FEAT
    units = nz * ny * HID
    tokens = 2 * nx * 32
    vmem = pl.BlockSpec(memory_space=pltpu.VMEM)
    hbm = pl.BlockSpec(memory_space=pl.ANY)
    dma = pltpu.SemaphoreType.DMA
    return pl.pallas_call(
        functools.partial(body, sizes),
        name="moe_step",
        out_shape=jax.ShapeDtypeStruct((32, FEAT), BF16),
        in_specs=[vmem, vmem, vmem, hbm, hbm, hbm],
        out_specs=vmem,
        scratch_shapes=[
            pltpu.VMEM((2, nx, ny, nz, ROWS, 128), BF16),
            pltpu.VMEM((ny, nz, LOCAL, HID, CAP), BF16),
            pltpu.VMEM((2 * LOCAL, HID, features), BF16),
            pltpu.VMEM((nz * ny, 2, 128, 128), BF16),
            pltpu.VMEM((LOCAL, units, FEAT), BF16),
            pltpu.VMEM((2 * top, LOCAL, 64, 4 * ny * HID), BF16),
            pltpu.VMEM((256, 256), BF16),
            pltpu.VMEM((256, tokens // 2), F32),
            pltpu.VMEM((LOCAL, 64, CAP), F32),
            pltpu.VMEM((LOCAL, tokens, CAP), BF16),
            pltpu.VMEM((tokens, LOCAL * CAP), BF16),
            pltpu.VMEM((2 * nx, ROWS, 128), F32),
            pltpu.VMEM((2 * nx, ROWS, 128), F32),
            dma((3,)),
            dma((top + 1, 7)),
            dma((top + 1, 7)),
            dma((top + 1, 5)),
            dma((top + 1, 5)),
            dma((1,)),
            dma((1,)),
        ],
        compiler_params=pltpu.CompilerParams(
            collective_id=0, has_side_effects=True, vmem_limit_bytes=48 * 1024 * 1024
        ),
    )(*args)


def solution(mesh):
    nz, ny = 32, 4
    nx = mesh.shape["expert"] // 2
    torus = Mesh(mesh.devices.reshape(nx, 2, nz, ny), ("x", "c", "z", "y"))
    experts, tensor = ("x", "c"), ("z", "y")
    placed = (
        P(experts, tensor),
        P(experts, None),
        P(experts, None),
        P(experts, tensor, None),
        P(experts, tensor, None),
        P(experts, None, tensor),
    )
    return jax.shard_map(
        functools.partial(on_device, (nx, nz, ny)),
        mesh=torus, in_specs=placed, out_specs=P(experts, tensor), check_vma=False,
    )
```
